32 devices in a mesh: dp: 2 (over y), ep: 16 (over z, x, core).
Axes of the slice: x: 2, y: 2, z: 4, core: 2. Of those that a mesh axis runs over, the one named last changes fastest.
Arguments:
- hidden_in: bfloat16 [768, 4096], P(('dp', 'ep')), may hold values from -6 to 6
- expert_ids: int32 [768, 2], P(('dp', 'ep')), may hold values from 0 to 15, all different within a row; in each aligned block of 24 rows (0 to 23, 24 to 47, ...) at most 4 rows name the same one
- route_logits: float32 [768, 16], P(('dp', 'ep')), may hold values from -10 to 10
- first_weight: bfloat16 [16, 4096, 1024], P('ep', None, 'dp'), may hold values from -0.09375 to 0.09375
- second_weight: bfloat16 [16, 1024, 4096], P('ep', None, 'dp'), may hold values from -0.1875 to 0.1875
- queries: bfloat16 [768, 2048], P(('dp', 'ep')), may hold values from -140 to 140
- span_keys: bfloat16 [768, 2048], P(('dp', 'ep')), may hold values from -7 to 7
- span_values: bfloat16 [768, 2048], P(('dp', 'ep')), may hold values from -6 to 6
- cache_keys: bfloat16 [32, 72, 2048], P(('dp', 'ep')), may hold values from -6 to 6
- cache_values: bfloat16 [32, 72, 2048], P(('dp', 'ep')), may hold values from -6 to 6
- valid_frames: int32 [32], P(('dp', 'ep')), may hold values from 1 to 3
Outputs:
- mixed: bfloat16 [768, 4096], P(('dp', 'ep'))
- attended: bfloat16 [768, 2048], P(('dp', 'ep'))
The draws below stay inside these ranges and needn't reach their ends.
Inputs may be any that keep to these rules, and one draw needn't show every extreme that they name: `expert_ids`: each token names two different experts. In the rows of one device (24 rows) no expert is named more than 4 times, a bound that some block reaches.
All inputs are finite; a program needn't handle non-finite values.
Results may differ from the reference program's by a relative error of at most 0.0057.
Values may be sent and summed in bfloat16 or wider, within the bound.
A program may use at most 128 MiB of HBM per device.

```python
import math
import jax
import jax.numpy as jnp
import numpy as np
from jax import lax

D = 4096
FFN = 1024
HEADS = 16
HEAD_DIM = 128
TOK = 24
FRAME_TOK = 24
CFRAMES = 3
CACHE_TOK = 72
EXPERTS = 16
STREAMS = 32
TOKENS = 768
CAP = 4


def query_key_pair(key):
    width = HEADS * HEAD_DIM
    key_rows = jnp.clip(jax.random.normal(jax.random.fold_in(key, 101), (TOKENS, width), jnp.float32), -6.0, 6.0)
    query_rows = jnp.clip(jax.random.normal(jax.random.fold_in(key, 202), (TOKENS, width), jnp.float32), -6.0, 6.0)
    return (query_rows, key_rows)


def draw_queries(key, part):
    query_rows, key_rows = query_key_pair(key)
    return query_rows.astype(jnp.bfloat16)


def draw_span_keys(key, part):
    query_rows, key_rows = query_key_pair(key)
    return key_rows.astype(jnp.bfloat16)


def set_ends(entries, own_key, low, largest):
    longest = entries.shape.index(max(entries.shape))
    spots = []
    for shift in (0, 1):
        where = [jax.random.randint(jax.random.fold_in(own_key, axis), (), 0, length) for axis, length in enumerate(entries.shape)]
        where[longest] = (where[longest] + shift) % entries.shape[longest]
        spots.append(tuple(where))
    return entries.at[spots[0]].set(low).at[spots[1]].set(largest)


def steps_of(stream_key, dims, pieces, low, high):
    loudness, own = 1.0, jax.random.fold_in(stream_key, 6)
    for dim, shards_of in pieces:
        steps = jnp.exp(jax.random.uniform(jax.random.fold_in(own, dim), (shards_of,), jnp.float32, low / len(pieces), high / len(pieces)))
        loudness = loudness * jnp.repeat(steps, dims[dim] // shards_of).reshape([-1 if axis == dim else 1 for axis in range(len(dims))])
    return loudness


def assign_block(stream_key, own, number, rows, count, top, reach, lean):
    ranking = jax.random.permutation(stream_key, count)
    crowded, ordinary = load_shares(count, rows * top, reach, lean, True), load_shares(count, rows * top, reach, lean, False)
    places = jnp.arange(count)

    def named(lengths, offset_by):
        used = int((lengths > 0).sum())
        fixed = max(1, used // 4)
        passed = fixed + (places - fixed + offset_by * (used - fixed)) % max(1, count - fixed)
        return jnp.zeros((count,), jnp.int32).at[ranking[jnp.where(places < fixed, places, passed)]].set(jnp.asarray(lengths, jnp.int32))

    lengths = jnp.where(number % 4 == 0, named(crowded, number // 4), named(ordinary, number - number // 4 - 1))
    mixed = jax.random.permutation(jax.random.fold_in(own, 3), count)
    giver, receiver = mixed[0:count // 2 * 2:2], mixed[1:count // 2 * 2:2]
    margin = jnp.minimum(lengths[giver] - 1, reach - lengths[receiver]) // 2
    margin = jnp.where((giver == ranking[0]) | (receiver == ranking[0]) | (lengths[receiver] == 0), 0, jnp.maximum(margin, 0))
    passed = jax.random.randint(jax.random.fold_in(own, 4), (count // 2,), 0, 1 << 20) % (margin + 1)
    lengths = lengths.at[giver].add(-passed).at[receiver].add(passed)
    members = jnp.searchsorted(jnp.cumsum(lengths), jnp.arange(rows * top), side="right").astype(jnp.int32)
    listing = members.reshape(top, rows).T
    listing = listing[jax.random.permutation(jax.random.fold_in(own, 1), rows)]
    offset_by = jax.random.randint(jax.random.fold_in(own, 2), (rows, 1), 0, top)
    return jnp.take_along_axis(listing, (jnp.arange(top)[None, :] + offset_by) % top, axis=1)


def load_shares(amount, total, bound, lean, full):
    portions = [(1 << 20) // math.isqrt(rank ** lean) + 1 for rank in range(1, amount + 1)]
    largest = bound if full else min(bound, max(-(-total // amount), total * portions[0] // sum(portions)))
    least = 1 if total - largest >= amount - 1 else 0
    given, surplus = [largest] + [least] * (amount - 1), total - largest - least * (amount - 1)
    while surplus > 0:
        candidates = [i for i in range(1, amount) if given[i] < largest] or [i for i in range(1, amount) if given[i] < bound]
        pool, left = sum([portions[i] for i in candidates]), surplus
        for i in candidates:
            extra = min(bound - given[i], max(1, left * portions[i] // pool), surplus)
            given[i] = given[i] + extra
            surplus = surplus - extra
    return np.array(given)


def centred(key, extent, deviation, limit, pieces=(), kind=jnp.bfloat16):
    array = deviation * jax.random.normal(key, extent, jnp.float32)
    if pieces:
        array = array * steps_of(key, extent, pieces, -0.22, 0.18)
    return jnp.clip(array, -limit, limit).astype(kind)


def setup_inputs(seed: int = 0) -> dict:
    key_list = jax.random.split(jax.random.key(seed), 12)
    hidden_in = centred(key_list[0], (TOKENS, D), 1.0, 6.0, ((0, 32),))
    expert_ids_keys = jax.random.split(jax.random.fold_in(key_list[1], 1), TOKENS // TOK)
    expert_ids_turns = jax.random.permutation(jax.random.fold_in(key_list[1], 3), TOKENS // TOK)
    expert_ids = jax.vmap(lambda own, number: assign_block(jax.random.fold_in(key_list[1], 2), own, number, TOK, EXPERTS, 2, CAP, 2))(expert_ids_keys, expert_ids_turns).reshape((TOKENS, 2))
    route_logits = centred(key_list[2], (TOKENS, EXPERTS), 2.0, 10.0, ((0, 32),), jnp.float32)
    first_weight = centred(key_list[3], (EXPERTS, D, FFN), D ** -0.5, 0.09375, ((0, 16), (2, 2)))
    second_weight = centred(key_list[4], (EXPERTS, FFN, D), FFN ** -0.5, 0.1875, ((0, 16), (2, 2)))
    queries = draw_queries(jax.random.fold_in(key_list[11], 71), 0)
    span_keys = draw_span_keys(jax.random.fold_in(key_list[11], 71), 0)
    span_values = centred(key_list[7], (TOKENS, HEADS * HEAD_DIM), 1.0, 6.0, ((0, 32),))
    cache_keys = centred(key_list[8], (STREAMS, CACHE_TOK, HEADS * HEAD_DIM), 1.0, 6.0, ((0, 32),))
    cache_values = centred(key_list[9], (STREAMS, CACHE_TOK, HEADS * HEAD_DIM), 1.0, 6.0, ((0, 32),))
    valid_frames = set_ends(jax.random.randint(key_list[10], (STREAMS,), 1, CFRAMES + 1), jax.random.fold_in(key_list[10], 1), 1, CFRAMES).astype(jnp.int32)
    return dict(hidden_in=hidden_in, expert_ids=expert_ids, route_logits=route_logits, first_weight=first_weight, second_weight=second_weight, queries=queries, span_keys=span_keys, span_values=span_values, cache_keys=cache_keys, cache_values=cache_values, valid_frames=valid_frames)


def activate(pre):
    return jax.nn.gelu(pre, approximate=True).astype(jnp.bfloat16)

def attend(queries, span_keys, span_values, cache_keys, cache_values, valid_count):
    token_count = queries.shape[0]
    cache_len = cache_keys.shape[0]
    key_rows = jnp.concatenate([cache_keys, span_keys], axis=0)
    value_rows = jnp.concatenate([cache_values, span_values], axis=0)
    query_heads = queries.reshape(token_count, HEADS, HEAD_DIM).astype(jnp.float32)
    key_heads = key_rows.reshape(-1, HEADS, HEAD_DIM).astype(jnp.float32)
    value_heads = value_rows.reshape(-1, HEADS, HEAD_DIM).astype(jnp.float32)
    scores = jnp.einsum('thd,khd->htk', query_heads, key_heads) * (1.0 / math.sqrt(HEAD_DIM))
    position = jnp.arange(key_rows.shape[0], dtype=jnp.int32)
    usable = (position >= cache_len) | (position // FRAME_TOK < valid_count)
    scores = jnp.where(usable[None, None, :], scores, -1e+30)
    row_max = lax.optimization_barrier(jnp.max(scores, axis=2, keepdims=True))
    weights = jnp.exp(scores - row_max)
    weights = (weights / lax.optimization_barrier(jnp.sum(weights, axis=2, keepdims=True))).astype(jnp.bfloat16)
    result = jnp.einsum('htk,khd->thd', weights.astype(jnp.float32), value_heads)
    return result.astype(jnp.bfloat16).reshape(token_count, HEADS * HEAD_DIM)

def block_slots(expert_ids):
    assigned = TOK * 2
    blocks = expert_ids.reshape(STREAMS, assigned)
    row_ids = lax.broadcasted_iota(jnp.int32, (assigned, assigned), 0)
    col_ids = lax.broadcasted_iota(jnp.int32, (assigned, assigned), 1)

    def per_block(flat_ids):
        same_expert = (flat_ids[:, None] == flat_ids[None, :]) & (col_ids < row_ids)
        return lax.optimization_barrier(jnp.sum(same_expert.astype(jnp.int32), axis=1))
    return jax.vmap(per_block)(blocks).reshape(TOKENS, 2)

def reference(hidden_in, expert_ids, route_logits, first_weight, second_weight, queries, span_keys, span_values, cache_keys, cache_values, valid_frames):
    slots = block_slots(expert_ids)
    token_index = jnp.arange(TOKENS, dtype=jnp.int32)
    stream_of = token_index // TOK
    rows_at = (stream_of[:, None] * CAP + slots).astype(jnp.int32)
    slot_table = jnp.full((EXPERTS, STREAMS * CAP), TOKENS, jnp.int32)
    slot_table = slot_table.at[expert_ids, rows_at].set(jnp.broadcast_to(token_index[:, None], (TOKENS, 2)))
    padded = jnp.concatenate([hidden_in, jnp.zeros((1, D), jnp.bfloat16)], axis=0)

    def apply_expert(operands):
        first_matrix, second_matrix, index_row = operands
        expert_rows = padded[index_row]
        hidden = activate(jnp.dot(expert_rows, first_matrix, preferred_element_type=jnp.float32))
        return jnp.dot(hidden, second_matrix, preferred_element_type=jnp.float32).astype(jnp.bfloat16)
    expert_outs = lax.map(apply_expert, (first_weight, second_weight, slot_table))
    chosen = jnp.take_along_axis(route_logits, expert_ids, axis=1)
    gates = jax.nn.softmax(chosen, axis=1)
    running = jnp.zeros((TOKENS, D), jnp.float32)
    for column in range(2):
        picked = expert_outs[expert_ids[:, column], rows_at[:, column]].astype(jnp.float32)
        running = running + gates[:, column:column + 1] * picked
    mixed = running.astype(jnp.bfloat16)
    width = HEADS * HEAD_DIM
    attended = jax.vmap(attend)(queries.reshape(STREAMS, TOK, width), span_keys.reshape(STREAMS, TOK, width), span_values.reshape(STREAMS, TOK, width), cache_keys, cache_values, valid_frames).reshape(TOKENS, width)
    return (mixed, attended)
```

```python
import functools
import math

import jax
import jax.numpy as jnp
from jax import lax
from jax.experimental import pallas as pl
from jax.experimental.pallas import tpu as pltpu
from jax.sharding import PartitionSpec as P

HEAD_DIM = 128
FRAME_TOK = 24
TILE = 16
WAVES = 4
MESH = pl.DeviceIdType.MESH


def iota(shape, axis):
    return lax.broadcasted_iota(jnp.int32, shape, axis)


def as_bf16(mask):
    return jnp.where(mask, 1.0, 0.0).astype(jnp.bfloat16)


def log2(n):
    return n.bit_length() - 1


def fold_map(shape, long_axis, group, cap):
    long, tiled = iota(shape, long_axis), iota(shape, 1 - long_axis)
    fold = long >> log2(group * cap)
    source = (long & (group * cap - 1)) >> log2(cap)
    slot = long & (cap - 1)
    return as_bf16(tiled == source * TILE + fold * cap + slot)


def dot(a, b):
    return jnp.dot(a, b, preferred_element_type=jnp.float32)


def drain(view, sem):
    pltpu.make_async_copy(view, view, sem).wait()


def loop(low, high, body):
    if high - low <= 8:
        for i in range(low, high):
            body(i)
    else:
        lax.fori_loop(low, high, lambda i, carry: (body(i), carry)[1], 0)


def attend(q, k, v, ck, cv, frames, out, head):
    cache_len = ck.shape[0]
    scale = 1.0 / math.sqrt(HEAD_DIM)
    usable = (iota((1, cache_len), 1) // FRAME_TOK) < frames
    contract = (((1,), (1,)), ((), ()))
    cols = slice(head * HEAD_DIM, (head + 1) * HEAD_DIM)
    query = q[:, cols]
    old = lax.dot_general(query, ck[:, cols], contract, preferred_element_type=jnp.float32)
    new = lax.dot_general(query, k[:, cols], contract, preferred_element_type=jnp.float32)
    old = jnp.where(usable, old * scale, -1e30)
    new = new * scale
    top = jnp.maximum(
        jnp.max(old, axis=1, keepdims=True), jnp.max(new, axis=1, keepdims=True)
    )
    old = jnp.exp(old - top)
    new = jnp.exp(new - top)
    total = jnp.sum(old, axis=1, keepdims=True) + jnp.sum(new, axis=1, keepdims=True)
    old = (old / total).astype(jnp.bfloat16)
    new = (new / total).astype(jnp.bfloat16)
    out[:, cols] = (dot(old, cv[:, cols]) + dot(new, v[:, cols])).astype(jnp.bfloat16)


def kernel(
    dp_n, ep_n, cap, back_folds,
    frames, ids_hbm, logits_hbm, hidden_hbm,
    q_hbm, k_hbm, v_hbm, ck_hbm, cv_hbm, w1_hbm, w2_hbm,
    mixed, attended,
    ids, logits, hidden, w1, w2, q, k, v, ck, cv,
    disp, rows, xs, hid, ys, back_out, back_in,
    load_sem, disp_send, disp_recv, relay_send, relay_recv,
    hid_send, hid_recv, back_send, back_recv, own_sem,
):
    d, me = lax.axis_index("dp"), lax.axis_index("ep")
    tokens = hidden.shape[0]
    folds = TILE // cap
    fold_cols = disp.shape[2]
    back_cols = back_in.shape[2]
    total = dp_n * ep_n
    wave = ep_n // WAVES
    per, half = wave // 2, ep_n // 2
    slots = wave * cap
    own = per
    units = hid.shape[2]

    bits = [lax.rem(lax.div(me, jnp.int32(1 << b)), jnp.int32(2)) for b in range(log2(ep_n))]

    def partner(off):
        both = jnp.int32(0)
        for b, bit in enumerate(bits):
            both = both + (bit * ((off // (1 << b)) % 2)) * (1 << b)
        return me + off - 2 * both

    barrier = pltpu.get_barrier_semaphore()

    loads = [
        pltpu.make_async_copy(src, dst, load_sem.at[i])
        for i, (src, dst) in enumerate(
            [
                (ids_hbm, ids), (logits_hbm, logits), (hidden_hbm, hidden),
                (q_hbm, q), (k_hbm, k), (v_hbm, v), (ck_hbm, ck), (cv_hbm, cv),
                (w1_hbm, w1), (w2_hbm, w2),
            ]
        )
    ]
    for load in loads:
        load.start()

    def greet(off):
        pl.semaphore_signal(
            barrier, inc=1, device_id={"dp": d, "ep": partner(off)}, device_id_type=MESH
        )

    loop(1, ep_n, greet)
    for i in range(1, dp_n):
        pl.semaphore_signal(
            barrier,
            inc=1,
            device_id={"dp": lax.rem(d + i, jnp.int32(dp_n)), "ep": me},
            device_id_type=MESH,
        )
    for load in loads[:3]:
        load.wait()

    experts = iota((ep_n, tokens), 0)
    named = [experts == ids[c : c + 1, :] for c in range(2)]
    count = as_bf16(named[0] | named[1])
    earlier = as_bf16(iota((tokens, tokens), 0) < iota((tokens, tokens), 1))
    before = dot(count, earlier)
    eye = iota((tokens, tokens), 0) == iota((tokens, tokens), 1)
    place_row = []
    for c in range(2):
        slot = jnp.sum(jnp.where(named[c], before, 0.0), axis=0, keepdims=True).astype(jnp.int32)
        off = ids[c : c + 1, :] ^ me
        inner = off & (half - 1)
        at = (inner >> log2(per)) * wave + (inner & (per - 1)) + jnp.where(off < half, per, 0)
        place_row.append(at * TILE + slot)

    row_at = iota((wave * TILE, tokens), 0)

    def pick(w):
        pickers = [
            as_bf16(
                (row_at + (w * wave * TILE - f * cap) == place_row[0])
                | (row_at + (w * wave * TILE - f * cap) == place_row[1])
            )
            for f in range(folds)
        ]
        step = min(fold_cols, 256)
        for at in range(0, fold_cols, step):
            acc = dot(pickers[0], hidden[:, at : at + step])
            for f in range(1, folds):
                acc += dot(pickers[f], hidden[:, f * fold_cols + at : f * fold_cols + at + step])
            disp[w * wave : (w + 1) * wave, :, at : at + step] = acc.astype(jnp.bfloat16).reshape(
                wave, TILE, step
            )

    def send(p, off):
        pltpu.make_async_remote_copy(
            src_ref=disp.at[p],
            dst_ref=rows.at[d * ep_n + p],
            send_sem=disp_send,
            recv_sem=disp_recv.at[p],
            device_id={"dp": d, "ep": partner(off)},
            device_id_type=MESH,
        ).start()

    def pass_on(p, source):
        for j in range(1, dp_n):
            pltpu.make_async_remote_copy(
                src_ref=source,
                dst_ref=rows.at[d * ep_n + p],
                send_sem=relay_send,
                recv_sem=relay_recv.at[(p // wave) * dp_n + d],
                device_id={"dp": lax.rem(d + j, jnp.int32(dp_n)), "ep": me},
                device_id_type=MESH,
            ).start()

    def dispatch(w):
        loop(0, per, lambda i: send(w * wave + i, half + w * per + i))
        loop(1 if w == 0 else 0, per, lambda i: send(w * wave + per + i, w * per + i))
        if w == 0:
            pltpu.make_async_copy(disp.at[own], rows.at[d * ep_n + own], disp_recv.at[own]).start()
            pass_on(own, disp.at[own])

    def relay(w):
        def one(p):
            chunk = rows.at[d * ep_n + p]
            drain(chunk, disp_recv.at[p])
            pass_on(p, chunk)

        if w == 0:
            drain(rows.at[d * ep_n + own], disp_recv.at[own])
        loop(1 if w == 0 else 0, per, lambda i: one(w * wave + per + i))
        loop(0, per, lambda i: one(w * wave + i))

    unfold = fold_map((folds * slots, wave * TILE), 0, wave, cap)
    refold = fold_map((wave * TILE, back_folds * slots), 1, wave, cap)

    def first(w):
        for j in range(1, dp_n):
            plane = lax.rem(d + j, jnp.int32(dp_n))
            drain(rows.at[pl.ds(plane * ep_n + w * wave, wave)], relay_recv.at[w * dp_n + plane])
        for plane in range(dp_n):
            at = plane * ep_n + w * wave
            flat = dot(unfold, rows[at : at + wave].reshape(wave * TILE, fold_cols)).astype(jnp.bfloat16)
            for f in range(folds):
                xs[f, plane * slots : (plane + 1) * slots, :] = flat[f * slots : (f + 1) * slots]
        acc = dot(xs[0], w1[:fold_cols, :])
        for f in range(1, folds):
            acc += dot(xs[f], w1[f * fold_cols : (f + 1) * fold_cols, :])
        hid[w * dp_n + d] = jax.nn.gelu(acc, approximate=True).astype(jnp.bfloat16)
        for i in range(1, dp_n):
            pltpu.make_async_remote_copy(
                src_ref=hid.at[w * dp_n + d],
                dst_ref=hid.at[w * dp_n + d],
                send_sem=hid_send,
                recv_sem=hid_recv.at[w * dp_n + d],
                device_id={"dp": lax.rem(d + i, jnp.int32(dp_n)), "ep": me},
                device_id_type=MESH,
            ).start()

    def second(w):
        for i in range(1, dp_n):
            part = w * dp_n + lax.rem(d + i, jnp.int32(dp_n))
            drain(hid.at[part], hid_recv.at[part])
        for f in range(back_folds):
            cols = slice(f * back_cols, (f + 1) * back_cols)
            acc = dot(hid[w * dp_n], w2[:units, cols])
            for i in range(1, dp_n):
                acc += dot(hid[w * dp_n + i], w2[i * units : (i + 1) * units, cols])
            ys[f] = acc.astype(jnp.bfloat16)
        for plane in range(dp_n):
            flat = jnp.concatenate(
                [ys[f, plane * slots : (plane + 1) * slots, :] for f in range(back_folds)], axis=0
            )
            tiles = dot(refold, flat).astype(jnp.bfloat16)
            at = plane * ep_n + w * wave
            back_out[at : at + wave] = tiles.reshape(wave, TILE, back_cols)

        def give(p, off):
            for j in range(dp_n):
                plane = lax.rem(d + j, jnp.int32(dp_n))
                if isinstance(off, int) and off == 0 and j == 0:
                    continue
                pltpu.make_async_remote_copy(
                    src_ref=back_out.at[plane * ep_n + p],
                    dst_ref=back_in.at[d * ep_n + p],
                    send_sem=back_send,
                    recv_sem=back_recv,
                    device_id={"dp": plane, "ep": partner(off)},
                    device_id_type=MESH,
                ).start()

        loop(0, per, lambda i: give(w * wave + i, half + w * per + i))
        if w == 0:
            give(own, 0)
            pltpu.make_async_copy(
                back_out.at[d * ep_n + own], back_in.at[d * ep_n + own], own_sem
            ).start()
        loop(1 if w == 0 else 0, per, lambda i: give(w * wave + per + i, w * per + i))

    waiting = list(range(q.shape[1] // HEAD_DIM))

    def heads(n):
        for _ in range(min(n, len(waiting))):
            attend(q, k, v, ck, cv, frames[0], attended, waiting.pop(0))

    pick(0)
    pl.semaphore_wait(barrier, ep_n + dp_n - 2)
    dispatch(0)
    for w in range(1, WAVES):
        pick(w)
        dispatch(w)
    for load in loads[3:8]:
        load.wait()
    heads(8)
    relay(0)
    heads(4)
    relay(1)
    loads[8].wait()
    first(0)
    heads(2)
    relay(2)
    first(1)
    loads[9].wait()
    second(0)
    relay(3)
    first(2)
    second(1)
    first(3)
    second(2)
    heads(1)
    second(3)
    heads(len(waiting))

    chosen = [
        jnp.sum(jnp.where(named[c], logits[...], 0.0), axis=0, keepdims=True) for c in range(2)
    ]
    top = jnp.maximum(chosen[0], chosen[1])
    powers = [jnp.exp(x - top) for x in chosen]
    gates = [
        jnp.sum(jnp.where(eye, p / (powers[0] + powers[1]), 0.0), axis=1, keepdims=True)
        for p in powers
    ]
    place = [jnp.sum(jnp.where(eye, x, 0), axis=1, keepdims=True) for x in place_row]
    col_at = iota((tokens, ep_n * TILE), 1)
    picks = jnp.concatenate(
        [
            jnp.where(col_at - f * cap == place[c], 1.0, 0.0)
            for f in range(back_folds)
            for c in range(2)
        ],
        axis=0,
    ).astype(jnp.bfloat16)

    drain(back_in.at[pl.ds(0, total - 1)], back_recv)
    drain(back_in.at[0], own_sem)
    for h in range(dp_n):
        tiles = back_in[h * ep_n : (h + 1) * ep_n].reshape(ep_n * TILE, back_cols)
        picked = dot(picks, tiles)
        for f in range(back_folds):
            at = 2 * f * tokens
            cols = slice((h * back_folds + f) * back_cols, (h * back_folds + f + 1) * back_cols)
            mixed[:, cols] = (
                gates[0] * picked[at : at + tokens] + gates[1] * picked[at + tokens : at + 2 * tokens]
            ).astype(jnp.bfloat16)

    drain(disp.at[pl.ds(0, ep_n - 1)], disp_send)
    if dp_n > 1:
        drain(rows.at[pl.ds(0, (dp_n - 1) * ep_n)], relay_send)
        drain(hid.at[pl.ds(0, WAVES * (dp_n - 1))], hid_send)
    drain(back_out.at[pl.ds(0, total - 1)], back_send)


def shards(dp_n, ep_n, *args):
    (hidden_in, expert_ids, route_logits, first_weight, second_weight,
     queries, span_keys, span_values, cache_keys, cache_values, valid_frames) = args
    tokens, width = hidden_in.shape
    cap = max(2, 8 * tokens // (3 * ep_n))
    _, _, units = first_weight.shape
    _, all_units, cols = second_weight.shape
    folds = TILE // cap
    back_folds = min(folds, cols // 128)
    slots = dp_n * (ep_n // WAVES) * cap
    bf16 = jnp.bfloat16
    vmem, hbm = pl.BlockSpec(memory_space=pltpu.VMEM), pl.BlockSpec(memory_space=pltpu.HBM)
    dma = pltpu.SemaphoreType.DMA
    total = dp_n * ep_n
    streamed = (
        expert_ids.T, route_logits.T, hidden_in,
        queries, span_keys, span_values, cache_keys[0], cache_values[0],
        first_weight[0], second_weight[0],
    )
    return pl.pallas_call(
        functools.partial(kernel, dp_n, ep_n, cap, back_folds),
        out_shape=(
            jax.ShapeDtypeStruct((tokens, width), bf16),
            jax.ShapeDtypeStruct(queries.shape, bf16),
        ),
        in_specs=[pl.BlockSpec(memory_space=pltpu.SMEM)] + [hbm] * len(streamed),
        out_specs=(vmem, vmem),
        scratch_shapes=[
            pltpu.VMEM((2, tokens), jnp.int32),
            pltpu.VMEM((ep_n, tokens), jnp.float32),
            pltpu.VMEM((tokens, width), bf16),
            pltpu.VMEM((width, units), bf16),
            pltpu.VMEM((all_units, cols), bf16),
            pltpu.VMEM(queries.shape, bf16),
            pltpu.VMEM(span_keys.shape, bf16),
            pltpu.VMEM(span_values.shape, bf16),
            pltpu.VMEM(cache_keys.shape[1:], bf16),
            pltpu.VMEM(cache_values.shape[1:], bf16),
            pltpu.VMEM((ep_n, TILE, width // folds), bf16),
            pltpu.VMEM((total, TILE, width // folds), bf16),
            pltpu.VMEM((folds, slots, width // folds), bf16),
            pltpu.VMEM((WAVES * dp_n, slots, units), bf16),
            pltpu.VMEM((back_folds, slots, cols // back_folds), bf16),
            pltpu.VMEM((total, TILE, cols // back_folds), bf16),
            pltpu.VMEM((total, TILE, cols // back_folds), bf16),
            dma((len(streamed),)),
            dma(()),
            dma((ep_n,)),
            dma(()),
            dma((WAVES * dp_n,)),
            dma(()),
            dma((WAVES * dp_n,)),
            dma(()),
            dma(()),
            dma(()),
        ],
        compiler_params=pltpu.CompilerParams(
            collective_id=0, has_side_effects=True, vmem_limit_bytes=48 * 1024 * 1024
        ),
    )(
        valid_frames,
        *[pltpu.with_memory_space_constraint(x, pltpu.HBM) for x in streamed],
    )


def solution(mesh):
    tokens = P(("dp", "ep"), None)
    weights = P("ep", None, "dp")
    cache = P(("dp", "ep"), None, None)
    return jax.shard_map(
        functools.partial(shards, mesh.shape["dp"], mesh.shape["ep"]),
        mesh=mesh,
        in_specs=(
            tokens, tokens, tokens, weights, weights, tokens, tokens, tokens, cache, cache,
            P(("dp", "ep")),
        ),
        out_specs=(tokens, tokens),
        check_vma=False,
    )
```

```python
import functools
import math

import jax
import jax.numpy as jnp
from jax import lax
from jax.experimental import pallas as pl
from jax.experimental.pallas import tpu as pltpu
from jax.sharding import PartitionSpec as P

HEAD_DIM = 128
FRAME_TOK = 24
TILE = 16
WAVES = 4
BLOCK = 16
MESH = pl.DeviceIdType.MESH


def iota(shape, axis):
    return lax.broadcasted_iota(jnp.int32, shape, axis)


def as_bf16(mask):
    return jnp.where(mask, 1.0, 0.0).astype(jnp.bfloat16)


def log2(n):
    return n.bit_length() - 1


def fold_map(shape, long_axis, group, cap):
    long, tiled = iota(shape, long_axis), iota(shape, 1 - long_axis)
    fold = long >> log2(group * cap)
    source = (long & (group * cap - 1)) >> log2(cap)
    slot = long & (cap - 1)
    return as_bf16(tiled == source * TILE + fold * cap + slot)


def dot(a, b):
    return jnp.dot(a, b, preferred_element_type=jnp.float32)


def drain(view, sem):
    pltpu.make_async_copy(view, view, sem).wait()


def loop(low, high, body):
    if high - low <= 8:
        for i in range(low, high):
            body(i)
    else:
        lax.fori_loop(low, high, lambda i, carry: (body(i), carry)[1], 0)


def attend(q, k, v, ck, cv, frames, out, head):
    cache_len = ck.shape[0]
    scale = 1.0 / math.sqrt(HEAD_DIM)
    usable = (iota((1, cache_len), 1) // FRAME_TOK) < frames
    contract = (((1,), (1,)), ((), ()))
    cols = slice(head * HEAD_DIM, (head + 1) * HEAD_DIM)
    query = q[:, cols]
    old = lax.dot_general(query, ck[:, cols], contract, preferred_element_type=jnp.float32)
    new = lax.dot_general(query, k[:, cols], contract, preferred_element_type=jnp.float32)
    old = jnp.where(usable, old * scale, -1e30)
    new = new * scale
    top = jnp.maximum(
        jnp.max(old, axis=1, keepdims=True), jnp.max(new, axis=1, keepdims=True)
    )
    old = jnp.exp(old - top)
    new = jnp.exp(new - top)
    total = jnp.sum(old, axis=1, keepdims=True) + jnp.sum(new, axis=1, keepdims=True)
    old = (old / total).astype(jnp.bfloat16)
    new = (new / total).astype(jnp.bfloat16)
    out[:, cols] = (dot(old, cv[:, cols]) + dot(new, v[:, cols])).astype(jnp.bfloat16)


def kernel(
    dp_n, ep_n, cap, back_folds,
    frames, ids_hbm, logits_hbm, hidden_hbm,
    q_hbm, k_hbm, v_hbm, ck_hbm, cv_hbm, w1_hbm, w2_hbm,
    mixed, attended,
    ids, logits, hidden, w1, w2, q, k, v, ck, cv,
    disp, rows, xs, hid, ys, back_out, mid_in, back_in,
    load_sem, disp_send, disp_recv, relay_send, relay_recv,
    hid_send, hid_recv, mid_send, mid_recv, back_send, back_recv, own_sem,
):
    d, me = lax.axis_index("dp"), lax.axis_index("ep")
    tokens = hidden.shape[0]
    folds = TILE // cap
    fold_cols = disp.shape[2]
    back_cols = back_in.shape[2]
    total = dp_n * ep_n
    quarter, half = ep_n // 4, ep_n // 2
    wave, per = ep_n // WAVES, half // WAVES
    units = hid.shape[1] // dp_n

    bits = [lax.rem(lax.div(me, jnp.int32(1 << b)), jnp.int32(2)) for b in range(log2(ep_n))]
    inner = bits[-2] + bits[-1] - 2 * bits[-2] * bits[-1]
    others = [lax.rem(d + j, jnp.int32(dp_n)) for j in range(1, dp_n)]

    def partner(off):
        both = jnp.int32(0)
        for b, bit in enumerate(bits):
            both = both + (bit * ((off // (1 << b)) % 2)) * (1 << b)
        return me + off - 2 * both

    def far_target(g, i):
        return half + (i // per) * quarter + g * per + i % per

    def target(part, i):
        if part == 0:
            return (1 - inner) * far_target(0, i) + inner * (quarter + i)
        if part == 1:
            return i
        if part == 2:
            return (1 - inner) * (quarter + i) + inner * far_target(0, i)
        return far_target(1, i)

    def landing(off):
        lo = off % quarter
        far = off // half
        w = far * (2 * (lo // per) + inner) + (1 - far) * (off // per)
        return w * wave + far * per + lo % per

    def source(w, far, i):
        if not far:
            return w * per + i
        side = inner if w % 2 else 1 - inner
        return half + side * quarter + (w // 2) * per + i - per

    barrier = pltpu.get_barrier_semaphore()

    loads = [
        pltpu.make_async_copy(src, dst, load_sem.at[i])
        for i, (src, dst) in enumerate(
            [
                (ids_hbm, ids), (logits_hbm, logits), (hidden_hbm, hidden),
                (q_hbm, q), (k_hbm, k), (v_hbm, v), (ck_hbm, ck), (cv_hbm, cv),
                (w1_hbm, w1), (w2_hbm, w2),
            ]
        )
    ]
    for load in loads[:3]:
        load.start()

    def greet(off):
        pl.semaphore_signal(
            barrier, inc=1, device_id={"dp": d, "ep": partner(off)}, device_id_type=MESH
        )

    for plane in others:
        pl.semaphore_signal(barrier, inc=1, device_id={"dp": plane, "ep": me}, device_id_type=MESH)
    loop(1, ep_n, lambda i: greet(ep_n - i))
    for load in loads[3:]:
        load.start()
    for load in loads[:3]:
        load.wait()

    experts = iota((ep_n, tokens), 0)
    named = [experts == ids[c : c + 1, :] for c in range(2)]
    count = as_bf16(named[0] | named[1])
    earlier = as_bf16(iota((tokens, tokens), 0) < iota((tokens, tokens), 1))
    before = dot(count, earlier)
    eye = iota((tokens, tokens), 0) == iota((tokens, tokens), 1)
    place_row, back_row = [], []
    for c in range(2):
        slot = jnp.sum(jnp.where(named[c], before, 0.0), axis=0, keepdims=True).astype(jnp.int32)
        off = ids[c : c + 1, :] ^ me
        lo = off & (quarter - 1)
        side = (off >> log2(quarter)) & 1
        g = lo >> log2(per)
        far = (3 * g + (1 - g) * 2 * inner) * quarter + side * per + (lo & (per - 1))
        beside = lo + jnp.where(side > 0, 2 * (1 - inner), 1) * quarter
        at = jnp.where(off < half, beside, far)
        back_row.append(off * TILE + slot)
        place_row.append(at * TILE + slot)

    row_at = iota((quarter * TILE, tokens), 0)

    def pick(part):
        base = part * quarter
        pickers = [
            as_bf16(
                (row_at + (base * TILE - f * cap) == place_row[0])
                | (row_at + (base * TILE - f * cap) == place_row[1])
            )
            for f in range(folds)
        ]
        step = min(fold_cols, 256)
        for at in range(0, fold_cols, step):
            acc = dot(pickers[0], hidden[:, at : at + step])
            for f in range(1, folds):
                acc += dot(pickers[f], hidden[:, f * fold_cols + at : f * fold_cols + at + step])
            disp[base : base + quarter, :, at : at + step] = acc.astype(jnp.bfloat16).reshape(
                quarter, TILE, step
            )

    def pass_on(g, p, chunk):
        for plane in others:
            pltpu.make_async_remote_copy(
                src_ref=chunk,
                dst_ref=rows.at[d * ep_n + p],
                send_sem=relay_send,
                recv_sem=relay_recv.at[g * dp_n + d],
                device_id={"dp": plane, "ep": me},
                device_id_type=MESH,
            ).start()

    def dispatch(part):
        def send(i):
            off = target(part, i)
            p = landing(off)
            pltpu.make_async_remote_copy(
                src_ref=disp.at[part * quarter + i],
                dst_ref=rows.at[d * ep_n + p],
                send_sem=disp_send,
                recv_sem=disp_recv.at[p],
                device_id={"dp": d, "ep": partner(off)},
                device_id_type=MESH,
            ).start()

        if part == 1:
            pltpu.make_async_copy(disp.at[quarter], rows.at[d * ep_n], disp_recv.at[0]).start()
            pass_on(0, 0, disp.at[quarter])
        loop(1 if part == 1 else 0, quarter, send)

    def relay(w, far):
        def one(p):
            chunk = rows.at[d * ep_n + p]
            drain(chunk, disp_recv.at[p])
            pass_on(w, p, chunk)

        low = far * per
        if w == 0 and not far:
            drain(rows.at[d * ep_n], disp_recv.at[0])
            low = 1
        loop(low, (1 + far) * per, lambda i: one(w * wave + i))

    def blocks(g):
        at, n = g * wave, wave
        size = min(BLOCK, dp_n * n)
        for b in range(0, dp_n * n, size):
            if size < n:
                yield b, size, [(b // n * ep_n + at + b % n, size)]
            else:
                yield b, size, [((b // n + j) * ep_n + at, n) for j in range(size // n)]

    def first(g):
        at, n = g * wave, wave
        height = dp_n * n * cap
        for plane in others:
            drain(rows.at[pl.ds(plane * ep_n + at, n)], relay_recv.at[g * dp_n + plane])
        for b, size, parts in blocks(g):
            unfold = fold_map((folds * size * cap, size * TILE), 0, size, cap)
            tiles = jnp.concatenate(
                [rows[lo : lo + m].reshape(m * TILE, fold_cols) for lo, m in parts], axis=0
            )
            flat = dot(unfold, tiles).astype(jnp.bfloat16)
            for f in range(folds):
                xs[b * cap : (b + size) * cap, f * fold_cols : (f + 1) * fold_cols] = flat[f * size * cap : (f + 1) * size * cap]
        acc = dot(xs[...], w1[...])
        here = (pl.ds(g * height, height), pl.ds(pl.multiple_of(d * units, 128), units))
        hid[here] = jax.nn.gelu(acc, approximate=True).astype(jnp.bfloat16)
        for plane in others:
            pltpu.make_async_remote_copy(
                src_ref=hid.at[here],
                dst_ref=hid.at[here],
                send_sem=hid_send,
                recv_sem=hid_recv.at[g * dp_n + d],
                device_id={"dp": plane, "ep": me},
                device_id_type=MESH,
            ).start()

    def hid_wait(g):
        height = dp_n * wave * cap
        for plane in others:
            part = hid.at[pl.ds(g * height, height), pl.ds(pl.multiple_of(plane * units, 128), units)]
            drain(part, hid_recv.at[g * dp_n + plane])

    def second(g):
        at, n = g * wave, wave
        height = dp_n * n * cap
        ys[...] = dot(hid[g * height : (g + 1) * height, :], w2[...]).astype(jnp.bfloat16)
        for b, size, parts in blocks(g):
            refold = fold_map((size * TILE, back_folds * size * cap), 1, size, cap)
            flat = jnp.concatenate(
                [
                    ys[b * cap : (b + size) * cap, f * back_cols : (f + 1) * back_cols]
                    for f in range(back_folds)
                ],
                axis=0,
            )
            tiles = dot(refold, flat).astype(jnp.bfloat16).reshape(size, TILE, back_cols)
            done = 0
            for lo, m in parts:
                back_out[lo : lo + m] = tiles[done : done + m]
                done += m
        give_back(g, back_out, d, d)
        if g == 0:
            pltpu.make_async_copy(back_out.at[d * ep_n], back_in.at[d * ep_n], own_sem).start()

    def give_back(g, tiles, plane, origin):
        at, n = g * wave, wave

        def give(far, i):
            off = source(g, far, i)
            pltpu.make_async_remote_copy(
                src_ref=tiles.at[plane * ep_n + at + i],
                dst_ref=back_in.at[origin * ep_n + off],
                send_sem=back_send,
                recv_sem=back_recv,
                device_id={"dp": d if tiles is mid_in else plane, "ep": partner(off)},
                device_id_type=MESH,
            ).start()

        loop(per, n, functools.partial(give, True))
        loop(1 if g == 0 else 0, per, functools.partial(give, False))

    def straight(g):
        for plane in others:
            give_back(g, back_out, plane, d)
            if g == 0:
                hand_over(plane)

    def hand_over(plane):
        pltpu.make_async_remote_copy(
            src_ref=back_out.at[plane * ep_n],
            dst_ref=back_in.at[d * ep_n],
            send_sem=back_send,
            recv_sem=back_recv,
            device_id={"dp": plane, "ep": me},
            device_id_type=MESH,
        ).start()

    def span(g, plane):
        at, n = g * wave, wave
        skip = 1 if g == 0 else 0
        return pl.ds(plane * ep_n + at + skip, n - skip)

    def across(g):
        for plane in others:
            pltpu.make_async_remote_copy(
                src_ref=back_out.at[span(g, plane)],
                dst_ref=mid_in.at[span(g, d)],
                send_sem=mid_send,
                recv_sem=mid_recv.at[g * dp_n + d],
                device_id={"dp": plane, "ep": me},
                device_id_type=MESH,
            ).start()
            if g == 0:
                hand_over(plane)
        bridged.append(g)

    def bring(g):
        for plane in others:
            drain(mid_in.at[span(g, plane)], mid_recv.at[g * dp_n + plane])
            give_back(g, mid_in, plane, plane)

    bridged = []
    waiting = list(range(q.shape[1] // HEAD_DIM))

    def heads(n):
        for _ in range(min(n, len(waiting))):
            attend(q, k, v, ck, cv, frames[0], attended, waiting.pop(0))

    pick(0)
    pl.semaphore_wait(barrier, ep_n + dp_n - 2)
    dispatch(0)
    for part in range(1, 4):
        pick(part)
        dispatch(part)
    for load in loads[3:8]:
        load.wait()
    heads(1)
    relay(0, 0)
    heads(1)
    relay(1, 0)
    heads(2)
    relay(0, 1)
    relay(2, 0)
    heads(2)
    loads[8].wait()
    relay(1, 1)
    first(0)
    relay(3, 0)
    relay(2, 1)
    first(1)
    loads[9].wait()
    hid_wait(0)
    second(0)
    relay(3, 1)
    straight(0)
    first(2)
    hid_wait(1)
    second(1)
    first(3)
    straight(1)
    hid_wait(2)
    second(2)
    hid_wait(3)
    straight(2)
    second(3)
    straight(3)
    heads(16)

    chosen = [
        jnp.sum(jnp.where(named[c], logits[...], 0.0), axis=0, keepdims=True) for c in range(2)
    ]
    top = jnp.maximum(chosen[0], chosen[1])
    powers = [jnp.exp(x - top) for x in chosen]
    gates = [
        jnp.sum(jnp.where(eye, p / (powers[0] + powers[1]), 0.0), axis=1, keepdims=True)
        for p in powers
    ]
    place = [jnp.sum(jnp.where(eye, x, 0), axis=1, keepdims=True) for x in back_row]
    col_at = iota((tokens, ep_n * TILE), 1)
    picks = jnp.concatenate(
        [
            jnp.where(col_at - f * cap == place[c], 1.0, 0.0)
            for f in range(back_folds)
            for c in range(2)
        ],
        axis=0,
    ).astype(jnp.bfloat16)

    drain(back_in.at[pl.ds(0, total - 1)], back_recv)
    drain(back_in.at[0], own_sem)
    for h in range(dp_n):
        tiles = back_in[h * ep_n : (h + 1) * ep_n].reshape(ep_n * TILE, back_cols)
        picked = dot(picks, tiles)
        for f in range(back_folds):
            at = 2 * f * tokens
            cols = slice((h * back_folds + f) * back_cols, (h * back_folds + f + 1) * back_cols)
            mixed[:, cols] = (
                gates[0] * picked[at : at + tokens] + gates[1] * picked[at + tokens : at + 2 * tokens]
            ).astype(jnp.bfloat16)

    drain(disp.at[pl.ds(0, ep_n - 1)], disp_send)
    if dp_n > 1:
        drain(rows.at[pl.ds(0, (dp_n - 1) * ep_n)], relay_send)
        drain(hid.at[:, pl.ds(0, (dp_n - 1) * units)], hid_send)
        passed = sum(wave - (g == 0) for g in bridged)
        drain(mid_in.at[pl.ds(0, (dp_n - 1) * passed)], mid_send)
    drain(back_out.at[pl.ds(0, total - 1)], back_send)


def shards(dp_n, ep_n, *args):
    (hidden_in, expert_ids, route_logits, first_weight, second_weight,
     queries, span_keys, span_values, cache_keys, cache_values, valid_frames) = args
    tokens, width = hidden_in.shape
    cap = max(2, 8 * tokens // (3 * ep_n))
    _, _, units = first_weight.shape
    _, all_units, cols = second_weight.shape
    folds = TILE // cap
    back_folds = min(folds, cols // 128)
    bf16 = jnp.bfloat16
    vmem, hbm = pl.BlockSpec(memory_space=pltpu.VMEM), pl.BlockSpec(memory_space=pltpu.HBM)
    dma = pltpu.SemaphoreType.DMA
    total = dp_n * ep_n
    height = total * cap
    streamed = (
        expert_ids.T, route_logits.T, hidden_in,
        queries, span_keys, span_values, cache_keys[0], cache_values[0],
        first_weight[0], second_weight[0],
    )
    return pl.pallas_call(
        functools.partial(kernel, dp_n, ep_n, cap, back_folds),
        out_shape=(
            jax.ShapeDtypeStruct((tokens, width), bf16),
            jax.ShapeDtypeStruct(queries.shape, bf16),
        ),
        in_specs=[pl.BlockSpec(memory_space=pltpu.SMEM)] + [hbm] * len(streamed),
        out_specs=(vmem, vmem),
        scratch_shapes=[
            pltpu.VMEM((2, tokens), jnp.int32),
            pltpu.VMEM((ep_n, tokens), jnp.float32),
            pltpu.VMEM((tokens, width), bf16),
            pltpu.VMEM((width, units), bf16),
            pltpu.VMEM((all_units, cols), bf16),
            pltpu.VMEM(queries.shape, bf16),
            pltpu.VMEM(span_keys.shape, bf16),
            pltpu.VMEM(span_values.shape, bf16),
            pltpu.VMEM(cache_keys.shape[1:], bf16),
            pltpu.VMEM(cache_values.shape[1:], bf16),
            pltpu.VMEM((ep_n, TILE, width // folds), bf16),
            pltpu.VMEM((total, TILE, width // folds), bf16),
            pltpu.VMEM((height // WAVES, width), bf16),
            pltpu.VMEM((height, dp_n * units), bf16),
            pltpu.VMEM((height // WAVES, cols), bf16),
            pltpu.VMEM((total, TILE, cols // back_folds), bf16),
            pltpu.VMEM((total, TILE, cols // back_folds), bf16),
            pltpu.VMEM((total, TILE, cols // back_folds), bf16),
            dma((len(streamed),)),
            dma(()),
            dma((ep_n,)),
            dma(()),
            dma((WAVES * dp_n,)),
            dma(()),
            dma((WAVES * dp_n,)),
            dma(()),
            dma((WAVES * dp_n,)),
            dma(()),
            dma(()),
            dma(()),
        ],
        compiler_params=pltpu.CompilerParams(
            collective_id=0, has_side_effects=True, vmem_limit_bytes=44 * 1024 * 1024
        ),
    )(
        valid_frames,
        *[pltpu.with_memory_space_constraint(x, pltpu.HBM) for x in streamed],
    )


def solution(mesh):
    tokens = P(("dp", "ep"), None)
    weights = P("ep", None, "dp")
    cache = P(("dp", "ep"), None, None)
    return jax.shard_map(
        functools.partial(shards, mesh.shape["dp"], mesh.shape["ep"]),
        mesh=mesh,
        in_specs=(
            tokens, tokens, tokens, weights, weights, tokens, tokens, tokens, cache, cache,
            P(("dp", "ep")),
        ),
        out_specs=(tokens, tokens),
        check_vma=False,
    )
```

```python
import functools
import math

import jax
import jax.numpy as jnp
from jax import lax
from jax.experimental import pallas as pl
from jax.experimental.pallas import tpu as pltpu
from jax.sharding import PartitionSpec as P

HEAD_DIM = 128
FRAME_TOK = 24
TILE = 16
MICRO = 8
GROUPS = ((0, 1), (1, 1), (2, 2), (4, 2), (6, 2))
NEAR = (0, 1, 4, 5, 6, 7, 2, 3)
BLOCK = 16
MESH = pl.DeviceIdType.MESH


def iota(shape, axis):
    return lax.broadcasted_iota(jnp.int32, shape, axis)


def as_bf16(mask):
    return jnp.where(mask, 1.0, 0.0).astype(jnp.bfloat16)


def log2(n):
    return n.bit_length() - 1


def fold_map(shape, long_axis, group, cap):
    long, tiled = iota(shape, long_axis), iota(shape, 1 - long_axis)
    fold = long >> log2(group * cap)
    source = (long & (group * cap - 1)) >> log2(cap)
    slot = long & (cap - 1)
    return as_bf16(tiled == source * TILE + fold * cap + slot)


def dot(a, b):
    return jnp.dot(a, b, preferred_element_type=jnp.float32)


def drain(view, sem):
    pltpu.make_async_copy(view, view, sem).wait()


def loop(low, high, body):
    if high - low <= 8:
        for i in range(low, high):
            body(i)
    else:
        lax.fori_loop(low, high, lambda i, carry: (body(i), carry)[1], 0)


def attend(q, k, v, ck, cv, frames, out, head):
    cache_len = ck.shape[0]
    scale = 1.0 / math.sqrt(HEAD_DIM)
    usable = (iota((1, cache_len), 1) // FRAME_TOK) < frames
    contract = (((1,), (1,)), ((), ()))
    cols = slice(head * HEAD_DIM, (head + 1) * HEAD_DIM)
    query = q[:, cols]
    old = lax.dot_general(query, ck[:, cols], contract, preferred_element_type=jnp.float32)
    new = lax.dot_general(query, k[:, cols], contract, preferred_element_type=jnp.float32)
    old = jnp.where(usable, old * scale, -1e30)
    new = new * scale
    top = jnp.maximum(
        jnp.max(old, axis=1, keepdims=True), jnp.max(new, axis=1, keepdims=True)
    )
    old = jnp.exp(old - top)
    new = jnp.exp(new - top)
    total = jnp.sum(old, axis=1, keepdims=True) + jnp.sum(new, axis=1, keepdims=True)
    old = (old / total).astype(jnp.bfloat16)
    new = (new / total).astype(jnp.bfloat16)
    out[:, cols] = (dot(old, cv[:, cols]) + dot(new, v[:, cols])).astype(jnp.bfloat16)


def kernel(
    dp_n, ep_n, cap, back_folds,
    frames, ids_hbm, logits_hbm, hidden_hbm,
    q_hbm, k_hbm, v_hbm, ck_hbm, cv_hbm, w1_hbm, w2_hbm,
    mixed, attended,
    ids, logits, hidden, w1, w2, q, k, v, ck, cv,
    disp, rows, xs, hid, ys, back_out, mid_in, back_in,
    load_sem, disp_send, disp_recv, relay_send, relay_recv,
    hid_send, hid_recv, mid_send, mid_recv, back_send, back_recv, own_sem,
):
    d, me = lax.axis_index("dp"), lax.axis_index("ep")
    tokens = hidden.shape[0]
    folds = TILE // cap
    fold_cols = disp.shape[2]
    back_cols = back_in.shape[2]
    total = dp_n * ep_n
    quarter, half = ep_n // 4, ep_n // 2
    wave, per = ep_n // MICRO, half // MICRO
    starts = [m * wave for m, _ in GROUPS]
    counts = [n * wave for _, n in GROUPS]
    group_of = [g for g, (_, n) in enumerate(GROUPS) for _ in range(n)]
    units = hid.shape[1] // dp_n

    bits = [lax.rem(lax.div(me, jnp.int32(1 << b)), jnp.int32(2)) for b in range(log2(ep_n))]
    inner = bits[-2] + bits[-1] - 2 * bits[-2] * bits[-1]
    others = [lax.rem(d + j, jnp.int32(dp_n)) for j in range(1, dp_n)]

    def partner(off):
        both = jnp.int32(0)
        for b, bit in enumerate(bits):
            both = both + (bit * ((off // (1 << b)) % 2)) * (1 << b)
        return me + off - 2 * both

    def far_target(g, i):
        side = i // per % 2
        return half + side * quarter + g * 2 * per + i // (2 * per) * per + i % per

    def target(part, i):
        if part == 0:
            return (1 - inner) * far_target(0, i) + inner * (quarter + i)
        if part == 1:
            return i
        if part == 2:
            return (1 - inner) * (quarter + i) + inner * far_target(0, i)
        return far_target(1, i)

    def landing(off):
        lo = off % quarter
        far = off // half
        block = off // per
        turn = block // 2 % 2 * (1 - block // 4)
        near = (block - block // 4 * 2 + turn * 4) * wave + off % per
        micro = lo // (2 * per) * 4 + inner * 2 + lo // per % 2
        return far * (micro * wave + per + lo % per) + (1 - far) * near

    def source(micro, far, i):
        if not far:
            return NEAR[micro] * per + i
        side = inner if micro // 2 % 2 else 1 - inner
        return half + side * quarter + micro // 4 * 2 * per + micro % 2 * per + i

    barrier = pltpu.get_barrier_semaphore()

    loads = [
        pltpu.make_async_copy(src, dst, load_sem.at[i])
        for i, (src, dst) in enumerate(
            [
                (ids_hbm, ids), (logits_hbm, logits), (hidden_hbm, hidden),
                (q_hbm, q), (k_hbm, k), (v_hbm, v), (ck_hbm, ck), (cv_hbm, cv),
                (w1_hbm, w1), (w2_hbm, w2),
            ]
        )
    ]
    for load in loads[:3]:
        load.start()

    def greet(off):
        pl.semaphore_signal(
            barrier, inc=1, device_id={"dp": d, "ep": partner(off)}, device_id_type=MESH
        )

    for plane in others:
        pl.semaphore_signal(barrier, inc=1, device_id={"dp": plane, "ep": me}, device_id_type=MESH)
    loop(1, ep_n, lambda i: greet(ep_n - i))
    for load in loads[3:]:
        load.start()
    for load in loads[:3]:
        load.wait()

    experts = iota((ep_n, tokens), 0)
    named = [experts == ids[c : c + 1, :] for c in range(2)]
    count = as_bf16(named[0] | named[1])
    earlier = as_bf16(iota((tokens, tokens), 0) < iota((tokens, tokens), 1))
    before = dot(count, earlier)
    eye = iota((tokens, tokens), 0) == iota((tokens, tokens), 1)
    place_row, back_row = [], []
    for c in range(2):
        slot = jnp.sum(jnp.where(named[c], before, 0.0), axis=0, keepdims=True).astype(jnp.int32)
        off = ids[c : c + 1, :] ^ me
        lo = off & (quarter - 1)
        side = (off >> log2(quarter)) & 1
        g = lo >> log2(2 * per)
        far = (3 * g + (1 - g) * 2 * inner) * quarter
        far += ((lo >> log2(per)) & 1) * 2 * per + side * per + (lo & (per - 1))
        beside = lo + jnp.where(side > 0, 2 * (1 - inner), 1) * quarter
        at = jnp.where(off < half, beside, far)
        back_row.append(off * TILE + slot)
        place_row.append(at * TILE + slot)

    row_at = iota((quarter * TILE, tokens), 0)

    def pick(part):
        base = part * quarter
        pickers = [
            as_bf16(
                (row_at + (base * TILE - f * cap) == place_row[0])
                | (row_at + (base * TILE - f * cap) == place_row[1])
            )
            for f in range(folds)
        ]
        step = min(fold_cols, 256)
        for at in range(0, fold_cols, step):
            acc = dot(pickers[0], hidden[:, at : at + step])
            for f in range(1, folds):
                acc += dot(pickers[f], hidden[:, f * fold_cols + at : f * fold_cols + at + step])
            disp[base : base + quarter, :, at : at + step] = acc.astype(jnp.bfloat16).reshape(
                quarter, TILE, step
            )

    def pass_on(g, p, chunk):
        for plane in others:
            pltpu.make_async_remote_copy(
                src_ref=chunk,
                dst_ref=rows.at[d * ep_n + p],
                send_sem=relay_send,
                recv_sem=relay_recv.at[g * dp_n + d],
                device_id={"dp": plane, "ep": me},
                device_id_type=MESH,
            ).start()

    def dispatch(part):
        def send(i):
            off = target(part, i)
            p = landing(off)
            pltpu.make_async_remote_copy(
                src_ref=disp.at[part * quarter + i],
                dst_ref=rows.at[d * ep_n + p],
                send_sem=disp_send,
                recv_sem=disp_recv.at[p],
                device_id={"dp": d, "ep": partner(off)},
                device_id_type=MESH,
            ).start()

        if part == 1:
            pltpu.make_async_copy(disp.at[quarter], rows.at[d * ep_n], disp_recv.at[0]).start()
            pass_on(0, 0, disp.at[quarter])
        loop(1 if part == 1 else 0, quarter, send)

    def relay(low, high, far):
        for micro in range(low, high):
            def one(i, micro=micro):
                p = micro * wave + i
                chunk = rows.at[d * ep_n + p]
                drain(chunk, disp_recv.at[p])
                pass_on(group_of[micro], p, chunk)

            first_one = far * per
            if micro == 0 and not far:
                drain(rows.at[d * ep_n], disp_recv.at[0])
                first_one = 1
            loop(first_one, (1 + far) * per, one)

    def blocks(g):
        at, n = starts[g], counts[g]
        size = min(BLOCK, dp_n * n)
        for b in range(0, dp_n * n, size):
            if size < n:
                yield b, size, [(b // n * ep_n + at + b % n, size)]
            else:
                yield b, size, [((b // n + j) * ep_n + at, n) for j in range(size // n)]

    def first(g):
        at, n = starts[g], counts[g]
        height = dp_n * n * cap
        for plane in others:
            drain(rows.at[pl.ds(plane * ep_n + at, n)], relay_recv.at[g * dp_n + plane])
        for b, size, parts in blocks(g):
            unfold = fold_map((folds * size * cap, size * TILE), 0, size, cap)
            tiles = jnp.concatenate(
                [rows[lo : lo + m].reshape(m * TILE, fold_cols) for lo, m in parts], axis=0
            )
            flat = dot(unfold, tiles).astype(jnp.bfloat16)
            for f in range(folds):
                xs[b * cap : (b + size) * cap, f * fold_cols : (f + 1) * fold_cols] = flat[f * size * cap : (f + 1) * size * cap]
        acc = dot(xs[:height, :], w1[...])
        here = (pl.ds(dp_n * at * cap, height), pl.ds(pl.multiple_of(d * units, 128), units))
        hid[here] = jax.nn.gelu(acc, approximate=True).astype(jnp.bfloat16)
        for plane in others:
            pltpu.make_async_remote_copy(
                src_ref=hid.at[here],
                dst_ref=hid.at[here],
                send_sem=hid_send,
                recv_sem=hid_recv.at[g * dp_n + d],
                device_id={"dp": plane, "ep": me},
                device_id_type=MESH,
            ).start()

    def hid_wait(g):
        height, low = dp_n * counts[g] * cap, dp_n * starts[g] * cap
        for plane in others:
            part = hid.at[pl.ds(low, height), pl.ds(pl.multiple_of(plane * units, 128), units)]
            drain(part, hid_recv.at[g * dp_n + plane])

    def second(g):
        at, n = starts[g], counts[g]
        height = dp_n * n * cap
        low = dp_n * at * cap
        ys[:height, :] = dot(hid[low : low + height, :], w2[...]).astype(jnp.bfloat16)
        for b, size, parts in blocks(g):
            refold = fold_map((size * TILE, back_folds * size * cap), 1, size, cap)
            flat = jnp.concatenate(
                [
                    ys[b * cap : (b + size) * cap, f * back_cols : (f + 1) * back_cols]
                    for f in range(back_folds)
                ],
                axis=0,
            )
            tiles = dot(refold, flat).astype(jnp.bfloat16).reshape(size, TILE, back_cols)
            done = 0
            for lo, m in parts:
                back_out[lo : lo + m] = tiles[done : done + m]
                done += m
        give_back(g, back_out, d, d)
        if g == 0:
            pltpu.make_async_copy(back_out.at[d * ep_n], back_in.at[d * ep_n], own_sem).start()

    def give_back(g, tiles, plane, origin):
        def give(p, off):
            pltpu.make_async_remote_copy(
                src_ref=tiles.at[plane * ep_n + p],
                dst_ref=back_in.at[origin * ep_n + off],
                send_sem=back_send,
                recv_sem=back_recv,
                device_id={"dp": d if tiles is mid_in else plane, "ep": partner(off)},
                device_id_type=MESH,
            ).start()

        for far in (True, False):
            for micro in range(GROUPS[g][0], sum(GROUPS[g])):
                low = 1 if micro == 0 and not far else 0
                at = micro * wave + far * per
                loop(low, per, lambda i, m=micro, f=far, a=at: give(a + i, source(m, f, i)))

    def straight(g):
        for plane in others:
            give_back(g, back_out, plane, d)
            if g == 0:
                hand_over(plane)

    def hand_over(plane):
        pltpu.make_async_remote_copy(
            src_ref=back_out.at[plane * ep_n],
            dst_ref=back_in.at[d * ep_n],
            send_sem=back_send,
            recv_sem=back_recv,
            device_id={"dp": plane, "ep": me},
            device_id_type=MESH,
        ).start()

    def span(g, plane):
        at, n = starts[g], counts[g]
        skip = 1 if g == 0 else 0
        return pl.ds(plane * ep_n + at + skip, n - skip)

    def across(g):
        for plane in others:
            pltpu.make_async_remote_copy(
                src_ref=back_out.at[span(g, plane)],
                dst_ref=mid_in.at[span(g, d)],
                send_sem=mid_send,
                recv_sem=mid_recv.at[g * dp_n + d],
                device_id={"dp": plane, "ep": me},
                device_id_type=MESH,
            ).start()
            if g == 0:
                hand_over(plane)
        bridged.append(g)

    def bring(g):
        for plane in others:
            drain(mid_in.at[span(g, plane)], mid_recv.at[g * dp_n + plane])
            give_back(g, mid_in, plane, plane)

    bridged = []
    waiting = list(range(q.shape[1] // HEAD_DIM))

    def heads(n):
        for _ in range(min(n, len(waiting))):
            attend(q, k, v, ck, cv, frames[0], attended, waiting.pop(0))

    pick(0)
    pl.semaphore_wait(barrier, ep_n + dp_n - 2)
    dispatch(0)
    for part in range(1, 4):
        pick(part)
        dispatch(part)
    for load in loads[3:8]:
        load.wait()
    heads(1)
    relay(0, 2, 0)
    heads(1)
    relay(6, 8, 0)
    heads(1)
    relay(0, 1, 1)
    heads(1)
    relay(1, 2, 1)
    heads(1)
    relay(2, 4, 0)
    relay(2, 4, 1)
    loads[8].wait()
    first(0)
    first(1)
    relay(4, 6, 0)
    relay(4, 6, 1)
    first(2)
    loads[9].wait()
    hid_wait(0)
    second(0)
    hid_wait(1)
    second(1)
    relay(6, 8, 1)
    first(3)
    straight(0)
    hid_wait(2)
    second(2)
    first(4)
    straight(1)
    hid_wait(3)
    second(3)
    straight(3)
    hid_wait(4)
    second(4)
    straight(2)
    straight(4)
    heads(16)

    chosen = [
        jnp.sum(jnp.where(named[c], logits[...], 0.0), axis=0, keepdims=True) for c in range(2)
    ]
    top = jnp.maximum(chosen[0], chosen[1])
    powers = [jnp.exp(x - top) for x in chosen]
    gates = [
        jnp.sum(jnp.where(eye, p / (powers[0] + powers[1]), 0.0), axis=1, keepdims=True)
        for p in powers
    ]
    place = [jnp.sum(jnp.where(eye, x, 0), axis=1, keepdims=True) for x in back_row]
    col_at = iota((tokens, ep_n * TILE), 1)
    picks = jnp.concatenate(
        [
            jnp.where(col_at - f * cap == place[c], 1.0, 0.0)
            for f in range(back_folds)
            for c in range(2)
        ],
        axis=0,
    ).astype(jnp.bfloat16)

    drain(back_in.at[pl.ds(0, total - 1)], back_recv)
    drain(back_in.at[0], own_sem)
    for h in range(dp_n):
        tiles = back_in[h * ep_n : (h + 1) * ep_n].reshape(ep_n * TILE, back_cols)
        picked = dot(picks, tiles)
        for f in range(back_folds):
            at = 2 * f * tokens
            cols = slice((h * back_folds + f) * back_cols, (h * back_folds + f + 1) * back_cols)
            mixed[:, cols] = (
                gates[0] * picked[at : at + tokens] + gates[1] * picked[at + tokens : at + 2 * tokens]
            ).astype(jnp.bfloat16)

    drain(disp.at[pl.ds(0, ep_n - 1)], disp_send)
    if dp_n > 1:
        drain(rows.at[pl.ds(0, (dp_n - 1) * ep_n)], relay_send)
        drain(hid.at[:, pl.ds(0, (dp_n - 1) * units)], hid_send)
        passed = sum(counts[g] - (g == 0) for g in bridged)
        drain(mid_in.at[pl.ds(0, (dp_n - 1) * passed)], mid_send)
    drain(back_out.at[pl.ds(0, total - 1)], back_send)


def write_out(*refs):
    *refs, sem = refs
    half = len(refs) // 2
    copies = [
        pltpu.make_async_copy(src, dst, sem.at[i])
        for i, (src, dst) in enumerate(zip(refs[:half], refs[half:]))
    ]
    for copy in copies:
        copy.start()
    for copy in copies:
        copy.wait()


def shards(dp_n, ep_n, *args):
    (hidden_in, expert_ids, route_logits, first_weight, second_weight,
     queries, span_keys, span_values, cache_keys, cache_values, valid_frames) = args
    tokens, width = hidden_in.shape
    cap = max(2, 8 * tokens // (3 * ep_n))
    _, _, units = first_weight.shape
    _, all_units, cols = second_weight.shape
    folds = TILE // cap
    back_folds = min(folds, cols // 128)
    bf16 = jnp.bfloat16
    vmem, hbm = pl.BlockSpec(memory_space=pltpu.VMEM), pl.BlockSpec(memory_space=pltpu.HBM)
    dma = pltpu.SemaphoreType.DMA
    total = dp_n * ep_n
    height = total * cap
    tall = max(n for _, n in GROUPS)
    streamed = (
        expert_ids.T, route_logits.T, hidden_in,
        queries, span_keys, span_values, cache_keys[0], cache_values[0],
        first_weight[0], second_weight[0],
    )
    results = pl.pallas_call(
        functools.partial(kernel, dp_n, ep_n, cap, back_folds),
        out_shape=(
            jax.ShapeDtypeStruct((tokens, width), bf16),
            jax.ShapeDtypeStruct(queries.shape, bf16),
        ),
        in_specs=[pl.BlockSpec(memory_space=pltpu.SMEM)] + [hbm] * len(streamed),
        out_specs=(vmem, vmem),
        scratch_shapes=[
            pltpu.VMEM((2, tokens), jnp.int32),
            pltpu.VMEM((ep_n, tokens), jnp.float32),
            pltpu.VMEM((tokens, width), bf16),
            pltpu.VMEM((width, units), bf16),
            pltpu.VMEM((all_units, cols), bf16),
            pltpu.VMEM(queries.shape, bf16),
            pltpu.VMEM(span_keys.shape, bf16),
            pltpu.VMEM(span_values.shape, bf16),
            pltpu.VMEM(cache_keys.shape[1:], bf16),
            pltpu.VMEM(cache_values.shape[1:], bf16),
            pltpu.VMEM((ep_n, TILE, width // folds), bf16),
            pltpu.VMEM((total, TILE, width // folds), bf16),
            pltpu.VMEM((height * tall // MICRO, width), bf16),
            pltpu.VMEM((height, dp_n * units), bf16),
            pltpu.VMEM((height * tall // MICRO, cols), bf16),
            pltpu.VMEM((total, TILE, cols // back_folds), bf16),
            pltpu.VMEM((total, TILE, cols // back_folds), bf16),
            pltpu.VMEM((total, TILE, cols // back_folds), bf16),
            dma((len(streamed),)),
            dma(()),
            dma((ep_n,)),
            dma(()),
            dma((len(GROUPS) * dp_n,)),
            dma(()),
            dma((len(GROUPS) * dp_n,)),
            dma(()),
            dma((len(GROUPS) * dp_n,)),
            dma(()),
            dma(()),
            dma(()),
        ],
        compiler_params=pltpu.CompilerParams(
            collective_id=0, has_side_effects=True, vmem_limit_bytes=44 * 1024 * 1024
        ),
    )(
        valid_frames,
        *[pltpu.with_memory_space_constraint(x, pltpu.HBM) for x in streamed],
    )
    return pl.pallas_call(
        write_out,
        out_shape=tuple(jax.ShapeDtypeStruct(x.shape, x.dtype) for x in results),
        in_specs=[pl.BlockSpec(memory_space=pl.ANY)] * len(results),
        out_specs=tuple([hbm] * len(results)),
        scratch_shapes=[dma((len(results),))],
    )(*[pltpu.with_memory_space_constraint(x, pltpu.VMEM) for x in results])


def solution(mesh):
    tokens = P(("dp", "ep"), None)
    weights = P("ep", None, "dp")
    cache = P(("dp", "ep"), None, None)
    return jax.shard_map(
        functools.partial(shards, mesh.shape["dp"], mesh.shape["ep"]),
        mesh=mesh,
        in_specs=(
            tokens, tokens, tokens, weights, weights, tokens, tokens, tokens, cache, cache,
            P(("dp", "ep")),
        ),
        out_specs=(tokens, tokens),
        check_vma=False,
    )
```

```python
import functools
import math

import jax
import jax.numpy as jnp
from jax import lax
from jax.experimental import pallas as pl
from jax.experimental.pallas import tpu as pltpu
from jax.sharding import PartitionSpec as P

HEAD_DIM = 128
FRAME_TOK = 24
TILE = 16
MICRO = 8
GROUPS = ((0, 2), (2, 2), (4, 2), (6, 1), (7, 1))
NEAR = (0, 1, 4, 5, 6, 7, 2, 3)
BLOCK = 16
MESH = pl.DeviceIdType.MESH


def iota(shape, axis):
    return lax.broadcasted_iota(jnp.int32, shape, axis)


def as_bf16(mask):
    return jnp.where(mask, 1.0, 0.0).astype(jnp.bfloat16)


def log2(n):
    return n.bit_length() - 1


def fold_map(shape, long_axis, group, cap):
    long, tiled = iota(shape, long_axis), iota(shape, 1 - long_axis)
    fold = long >> log2(group * cap)
    source = (long & (group * cap - 1)) >> log2(cap)
    slot = long & (cap - 1)
    return as_bf16(tiled == source * TILE + fold * cap + slot)


def dot(a, b):
    return jnp.dot(a, b, preferred_element_type=jnp.float32)


def drain(view, sem):
    pltpu.make_async_copy(view, view, sem).wait()


def loop(low, high, body):
    if high - low <= 8:
        for i in range(low, high):
            body(i)
    else:
        lax.fori_loop(low, high, lambda i, carry: (body(i), carry)[1], 0)


def attend(q, k, v, ck, cv, frames, out, head):
    cache_len = ck.shape[0]
    scale = 1.0 / math.sqrt(HEAD_DIM)
    usable = (iota((1, cache_len), 1) // FRAME_TOK) < frames
    contract = (((1,), (1,)), ((), ()))
    cols = slice(head * HEAD_DIM, (head + 1) * HEAD_DIM)
    query = q[:, cols]
    old = lax.dot_general(query, ck[:, cols], contract, preferred_element_type=jnp.float32)
    new = lax.dot_general(query, k[:, cols], contract, preferred_element_type=jnp.float32)
    old = jnp.where(usable, old * scale, -1e30)
    new = new * scale
    top = jnp.maximum(
        jnp.max(old, axis=1, keepdims=True), jnp.max(new, axis=1, keepdims=True)
    )
    old = jnp.exp(old - top)
    new = jnp.exp(new - top)
    total = jnp.sum(old, axis=1, keepdims=True) + jnp.sum(new, axis=1, keepdims=True)
    old = (old / total).astype(jnp.bfloat16)
    new = (new / total).astype(jnp.bfloat16)
    out[:, cols] = (dot(old, cv[:, cols]) + dot(new, v[:, cols])).astype(jnp.bfloat16)


def kernel(
    dp_n, ep_n, cap, back_folds,
    frames, ids_hbm, logits_hbm, hidden_hbm,
    q_hbm, k_hbm, v_hbm, ck_hbm, cv_hbm, w1_hbm, w2_hbm,
    mixed, attended,
    ids, logits, hidden, w1, w2, q, k, v, ck, cv,
    disp, rows, xs, hid, ys, back_out, back_in,
    load_sem, disp_send, disp_recv, relay_send, relay_recv,
    hid_send, hid_recv, back_send, back_recv, own_sem,
):
    d, me = lax.axis_index("dp"), lax.axis_index("ep")
    tokens = hidden.shape[0]
    folds = TILE // cap
    fold_cols = disp.shape[2]
    back_cols = back_in.shape[2]
    total = dp_n * ep_n
    quarter, half = ep_n // 4, ep_n // 2
    wave, per = ep_n // MICRO, half // MICRO
    starts = [m * wave for m, _ in GROUPS]
    counts = [n * wave for _, n in GROUPS]
    group_of = [g for g, (_, n) in enumerate(GROUPS) for _ in range(n)]
    units = hid.shape[1] // dp_n

    bits = [lax.rem(lax.div(me, jnp.int32(1 << b)), jnp.int32(2)) for b in range(log2(ep_n))]
    inner = bits[-2] + bits[-1] - 2 * bits[-2] * bits[-1]
    others = [lax.rem(d + j, jnp.int32(dp_n)) for j in range(1, dp_n)]

    def partner(off):
        both = jnp.int32(0)
        for b, bit in enumerate(bits):
            both = both + (bit * ((off // (1 << b)) % 2)) * (1 << b)
        return me + off - 2 * both

    def far_target(g, i):
        side = i // per % 2
        return half + side * quarter + g * 2 * per + i // (2 * per) * per + i % per

    def target(part, i):
        if part == 0:
            return (1 - inner) * far_target(0, i) + inner * (quarter + i)
        if part == 1:
            return i
        if part == 2:
            return (1 - inner) * (quarter + i) + inner * far_target(0, i)
        return far_target(1, i)

    def landing(off):
        lo = off % quarter
        far = off // half
        block = off // per
        turn = block // 2 % 2 * (1 - block // 4)
        near = (block - block // 4 * 2 + turn * 4) * wave + off % per
        micro = lo // (2 * per) * 4 + inner * 2 + lo // per % 2
        return far * (micro * wave + per + lo % per) + (1 - far) * near

    def source(micro, far, i):
        if not far:
            return NEAR[micro] * per + i
        side = inner if micro // 2 % 2 else 1 - inner
        return half + side * quarter + micro // 4 * 2 * per + micro % 2 * per + i

    barrier = pltpu.get_barrier_semaphore()

    loads = [
        pltpu.make_async_copy(src, dst, load_sem.at[i])
        for i, (src, dst) in enumerate(
            [
                (ids_hbm, ids), (logits_hbm, logits), (hidden_hbm, hidden),
                (q_hbm, q), (k_hbm, k), (v_hbm, v), (ck_hbm, ck), (cv_hbm, cv),
                (w1_hbm, w1), (w2_hbm, w2),
            ]
        )
    ]
    for load in loads[:3]:
        load.start()

    def greet(off):
        pl.semaphore_signal(
            barrier, inc=1, device_id={"dp": d, "ep": partner(off)}, device_id_type=MESH
        )

    for plane in others:
        pl.semaphore_signal(barrier, inc=1, device_id={"dp": plane, "ep": me}, device_id_type=MESH)
    loop(1, ep_n, lambda i: greet(ep_n - i))
    for load in loads[3:]:
        load.start()
    for load in loads[:3]:
        load.wait()

    experts = iota((ep_n, tokens), 0)
    named = [experts == ids[c : c + 1, :] for c in range(2)]
    count = as_bf16(named[0] | named[1])
    earlier = as_bf16(iota((tokens, tokens), 0) < iota((tokens, tokens), 1))
    before = dot(count, earlier)
    eye = iota((tokens, tokens), 0) == iota((tokens, tokens), 1)
    place_row, back_row = [], []
    for c in range(2):
        slot = jnp.sum(jnp.where(named[c], before, 0.0), axis=0, keepdims=True).astype(jnp.int32)
        off = ids[c : c + 1, :] ^ me
        lo = off & (quarter - 1)
        side = (off >> log2(quarter)) & 1
        g = lo >> log2(2 * per)
        far = (3 * g + (1 - g) * 2 * inner) * quarter
        far += ((lo >> log2(per)) & 1) * 2 * per + side * per + (lo & (per - 1))
        beside = lo + jnp.where(side > 0, 2 * (1 - inner), 1) * quarter
        at = jnp.where(off < half, beside, far)
        back_row.append(off * TILE + slot)
        place_row.append(at * TILE + slot)

    row_at = iota((quarter * TILE, tokens), 0)

    def pick(part):
        base = part * quarter
        pickers = [
            as_bf16(
                (row_at + (base * TILE - f * cap) == place_row[0])
                | (row_at + (base * TILE - f * cap) == place_row[1])
            )
            for f in range(folds)
        ]
        step = min(fold_cols, 256)
        for at in range(0, fold_cols, step):
            acc = dot(pickers[0], hidden[:, at : at + step])
            for f in range(1, folds):
                acc += dot(pickers[f], hidden[:, f * fold_cols + at : f * fold_cols + at + step])
            disp[base : base + quarter, :, at : at + step] = acc.astype(jnp.bfloat16).reshape(
                quarter, TILE, step
            )

    def pass_on(g, p, chunk):
        for j, plane in enumerate(others):
            pltpu.make_async_remote_copy(
                src_ref=chunk,
                dst_ref=rows.at[d * ep_n + p],
                send_sem=relay_send,
                recv_sem=relay_recv.at[(g + 1) * (dp_n - 1) - 1 - j],
                device_id={"dp": plane, "ep": me},
                device_id_type=MESH,
            ).start()

    def dispatch(part):
        def send(i):
            off = target(part, i)
            p = landing(off)
            pltpu.make_async_remote_copy(
                src_ref=disp.at[part * quarter + i],
                dst_ref=rows.at[d * ep_n + p],
                send_sem=disp_send,
                recv_sem=disp_recv.at[p],
                device_id={"dp": d, "ep": partner(off)},
                device_id_type=MESH,
            ).start()

        if part == 1:
            pltpu.make_async_copy(disp.at[quarter], rows.at[d * ep_n], disp_recv.at[0]).start()
            pass_on(0, 0, disp.at[quarter])
        loop(1 if part == 1 else 0, quarter, send)

    def relay(low, high, far):
        for micro in range(low, high):
            def one(i, micro=micro):
                p = micro * wave + i
                chunk = rows.at[d * ep_n + p]
                drain(chunk, disp_recv.at[p])
                pass_on(group_of[micro], p, chunk)

            first_one = far * per
            if micro == 0 and not far:
                drain(rows.at[d * ep_n], disp_recv.at[0])
                first_one = 1
            loop(first_one, (1 + far) * per, one)

    def blocks(g):
        at, n = starts[g], counts[g]
        size = min(BLOCK, dp_n * n)
        for b in range(0, dp_n * n, size):
            if size < n:
                yield b, size, [(b // n * ep_n + at + b % n, size)]
            else:
                yield b, size, [((b // n + j) * ep_n + at, n) for j in range(size // n)]

    def first(g):
        at, n = starts[g], counts[g]
        height = dp_n * n * cap
        for j, plane in enumerate(others):
            drain(rows.at[pl.ds(plane * ep_n + at, n)], relay_recv.at[g * (dp_n - 1) + j])
        for b, size, parts in blocks(g):
            unfold = fold_map((folds * size * cap, size * TILE), 0, size, cap)
            tiles = jnp.concatenate(
                [rows[lo : lo + m].reshape(m * TILE, fold_cols) for lo, m in parts], axis=0
            )
            flat = dot(unfold, tiles).astype(jnp.bfloat16)
            for f in range(folds):
                xs[b * cap : (b + size) * cap, f * fold_cols : (f + 1) * fold_cols] = flat[f * size * cap : (f + 1) * size * cap]
        acc = dot(xs[:height, :], w1[...])
        here = (pl.ds(dp_n * at * cap, height), pl.ds(pl.multiple_of(d * units, 128), units))
        hid[here] = jax.nn.gelu(acc, approximate=True).astype(jnp.bfloat16)
        for j, plane in enumerate(others):
            pltpu.make_async_remote_copy(
                src_ref=hid.at[here],
                dst_ref=hid.at[here],
                send_sem=hid_send,
                recv_sem=hid_recv.at[(g + 1) * (dp_n - 1) - 1 - j],
                device_id={"dp": plane, "ep": me},
                device_id_type=MESH,
            ).start()

    def hid_wait(g):
        height, low = dp_n * counts[g] * cap, dp_n * starts[g] * cap
        for j, plane in enumerate(others):
            part = hid.at[pl.ds(low, height), pl.ds(pl.multiple_of(plane * units, 128), units)]
            drain(part, hid_recv.at[g * (dp_n - 1) + j])

    def second(g):
        at, n = starts[g], counts[g]
        height = dp_n * n * cap
        low = dp_n * at * cap
        ys[:height, :] = dot(hid[low : low + height, :], w2[...]).astype(jnp.bfloat16)
        for b, size, parts in blocks(g):
            refold = fold_map((size * TILE, back_folds * size * cap), 1, size, cap)
            flat = jnp.concatenate(
                [
                    ys[b * cap : (b + size) * cap, f * back_cols : (f + 1) * back_cols]
                    for f in range(back_folds)
                ],
                axis=0,
            )
            tiles = dot(refold, flat).astype(jnp.bfloat16).reshape(size, TILE, back_cols)
            done = 0
            for lo, m in parts:
                back_out[lo : lo + m] = tiles[done : done + m]
                done += m
        give_back(g, d)
        if g == 0:
            pltpu.make_async_copy(back_out.at[d * ep_n], back_in.at[d * ep_n], own_sem).start()

    def give_back(g, plane):
        def give(p, off):
            pltpu.make_async_remote_copy(
                src_ref=back_out.at[plane * ep_n + p],
                dst_ref=back_in.at[d * ep_n + off],
                send_sem=back_send,
                recv_sem=back_recv,
                device_id={"dp": plane, "ep": partner(off)},
                device_id_type=MESH,
            ).start()

        for far in (True, False):
            for micro in range(GROUPS[g][0], sum(GROUPS[g])):
                low = 1 if micro == 0 and not far else 0
                at = micro * wave + far * per
                loop(low, per, lambda i, m=micro, f=far, a=at: give(a + i, source(m, f, i)))

    def straight(g):
        for plane in others:
            give_back(g, plane)
            if g == 0:
                hand_over(plane)

    def hand_over(plane):
        pltpu.make_async_remote_copy(
            src_ref=back_out.at[plane * ep_n],
            dst_ref=back_in.at[d * ep_n],
            send_sem=back_send,
            recv_sem=back_recv,
            device_id={"dp": plane, "ep": me},
            device_id_type=MESH,
        ).start()


    waiting = list(range(q.shape[1] // HEAD_DIM))

    def heads(n):
        for _ in range(min(n, len(waiting))):
            attend(q, k, v, ck, cv, frames[0], attended, waiting.pop(0))

    pick(0)
    pl.semaphore_wait(barrier, ep_n + dp_n - 2)
    dispatch(0)
    for part in range(1, 4):
        pick(part)
        dispatch(part)
    for load in loads[3:8]:
        load.wait()
    heads(1)
    relay(0, 2, 0)
    heads(1)
    relay(6, 8, 0)
    heads(1)
    relay(0, 1, 1)
    heads(1)
    relay(1, 2, 1)
    heads(1)
    relay(2, 4, 0)
    relay(2, 4, 1)
    loads[8].wait()
    first(0)
    relay(4, 6, 0)
    relay(4, 6, 1)
    first(1)
    loads[9].wait()
    hid_wait(0)
    second(0)
    relay(6, 8, 1)
    first(2)
    hid_wait(1)
    straight(0)
    second(1)
    first(3)
    first(4)
    hid_wait(2)
    second(2)
    straight(2)
    hid_wait(3)
    straight(1)
    second(3)
    hid_wait(4)
    straight(3)
    second(4)
    straight(4)
    heads(16)

    chosen = [
        jnp.sum(jnp.where(named[c], logits[...], 0.0), axis=0, keepdims=True) for c in range(2)
    ]
    top = jnp.maximum(chosen[0], chosen[1])
    powers = [jnp.exp(x - top) for x in chosen]
    gates = [
        jnp.sum(jnp.where(eye, p / (powers[0] + powers[1]), 0.0), axis=1, keepdims=True)
        for p in powers
    ]
    place = [jnp.sum(jnp.where(eye, x, 0), axis=1, keepdims=True) for x in back_row]
    col_at = iota((tokens, ep_n * TILE), 1)
    picks = jnp.concatenate(
        [
            jnp.where(col_at - f * cap == place[c], 1.0, 0.0)
            for f in range(back_folds)
            for c in range(2)
        ],
        axis=0,
    ).astype(jnp.bfloat16)

    drain(back_in.at[pl.ds(0, total - 1)], back_recv)
    drain(back_in.at[0], own_sem)
    for h in range(dp_n):
        tiles = back_in[h * ep_n : (h + 1) * ep_n].reshape(ep_n * TILE, back_cols)
        picked = dot(picks, tiles)
        for f in range(back_folds):
            at = 2 * f * tokens
            cols = slice((h * back_folds + f) * back_cols, (h * back_folds + f + 1) * back_cols)
            mixed[:, cols] = (
                gates[0] * picked[at : at + tokens] + gates[1] * picked[at + tokens : at + 2 * tokens]
            ).astype(jnp.bfloat16)

    drain(disp.at[pl.ds(0, ep_n - 1)], disp_send)
    if dp_n > 1:
        drain(rows.at[pl.ds(0, (dp_n - 1) * ep_n)], relay_send)
        drain(hid.at[:, pl.ds(0, (dp_n - 1) * units)], hid_send)
    drain(back_out.at[pl.ds(0, total - 1)], back_send)


def write_out(*refs):
    *refs, sem = refs
    half = len(refs) // 2
    copies = [
        pltpu.make_async_copy(src, dst, sem.at[i])
        for i, (src, dst) in enumerate(zip(refs[:half], refs[half:]))
    ]
    for copy in copies:
        copy.start()
    for copy in copies:
        copy.wait()


def shards(dp_n, ep_n, *args):
    (hidden_in, expert_ids, route_logits, first_weight, second_weight,
     queries, span_keys, span_values, cache_keys, cache_values, valid_frames) = args
    tokens, width = hidden_in.shape
    cap = max(2, 8 * tokens // (3 * ep_n))
    _, _, units = first_weight.shape
    _, all_units, cols = second_weight.shape
    folds = TILE // cap
    back_folds = min(folds, cols // 128)
    bf16 = jnp.bfloat16
    vmem, hbm = pl.BlockSpec(memory_space=pltpu.VMEM), pl.BlockSpec(memory_space=pltpu.HBM)
    dma = pltpu.SemaphoreType.DMA
    total = dp_n * ep_n
    height = total * cap
    tall = max(n for _, n in GROUPS)
    streamed = (
        expert_ids.T, route_logits.T, hidden_in,
        queries, span_keys, span_values, cache_keys[0], cache_values[0],
        first_weight[0], second_weight[0],
    )
    results = pl.pallas_call(
        functools.partial(kernel, dp_n, ep_n, cap, back_folds),
        out_shape=(
            jax.ShapeDtypeStruct((tokens, width), bf16),
            jax.ShapeDtypeStruct(queries.shape, bf16),
        ),
        in_specs=[pl.BlockSpec(memory_space=pltpu.SMEM)] + [hbm] * len(streamed),
        out_specs=(vmem, vmem),
        scratch_shapes=[
            pltpu.VMEM((2, tokens), jnp.int32),
            pltpu.VMEM((ep_n, tokens), jnp.float32),
            pltpu.VMEM((tokens, width), bf16),
            pltpu.VMEM((width, units), bf16),
            pltpu.VMEM((all_units, cols), bf16),
            pltpu.VMEM(queries.shape, bf16),
            pltpu.VMEM(span_keys.shape, bf16),
            pltpu.VMEM(span_values.shape, bf16),
            pltpu.VMEM(cache_keys.shape[1:], bf16),
            pltpu.VMEM(cache_values.shape[1:], bf16),
            pltpu.VMEM((ep_n, TILE, width // folds), bf16),
            pltpu.VMEM((total, TILE, width // folds), bf16),
            pltpu.VMEM((height * tall // MICRO, width), bf16),
            pltpu.VMEM((height, dp_n * units), bf16),
            pltpu.VMEM((height * tall // MICRO, cols), bf16),
            pltpu.VMEM((total, TILE, cols // back_folds), bf16),
            pltpu.VMEM((total, TILE, cols // back_folds), bf16),
            dma((len(streamed),)),
            dma(()),
            dma((ep_n,)),
            dma(()),
            dma((len(GROUPS) * max(1, dp_n - 1),)),
            dma(()),
            dma((len(GROUPS) * max(1, dp_n - 1),)),
            dma(()),
            dma(()),
            dma(()),
        ],
        compiler_params=pltpu.CompilerParams(
            collective_id=0, has_side_effects=True, vmem_limit_bytes=44 * 1024 * 1024
        ),
    )(
        valid_frames,
        *[pltpu.with_memory_space_constraint(x, pltpu.HBM) for x in streamed],
    )
    return pl.pallas_call(
        write_out,
        out_shape=tuple(jax.ShapeDtypeStruct(x.shape, x.dtype) for x in results),
        in_specs=[pl.BlockSpec(memory_space=pl.ANY)] * len(results),
        out_specs=tuple([hbm] * len(results)),
        scratch_shapes=[dma((len(results),))],
    )(*[pltpu.with_memory_space_constraint(x, pltpu.VMEM) for x in results])


def solution(mesh):
    tokens = P(("dp", "ep"), None)
    weights = P("ep", None, "dp")
    cache = P(("dp", "ep"), None, None)
    return jax.shard_map(
        functools.partial(shards, mesh.shape["dp"], mesh.shape["ep"]),
        mesh=mesh,
        in_specs=(
            tokens, tokens, tokens, weights, weights, tokens, tokens, tokens, cache, cache,
            P(("dp", "ep")),
        ),
        out_specs=(tokens, tokens),
        check_vma=False,
    )
```
